256 devices in a mesh: groups: 4 (over x, y), head: 32 (over z), seq: 2 (over core).
Axes of the slice: x: 2, y: 2, z: 32, core: 2. Of those that a mesh axis runs over, the one named last changes fastest.
The devices are a block of a 4x8x32 slice.
Arguments:
- hidden: bfloat16 [6144, 7168], P(('groups', 'head', 'seq')), parts along dimension 0, may hold values from -6 to 6
- query_latent: bfloat16 [6144, 1536], P(('groups', 'head', 'seq')), parts along dimension 0, may hold values from -240 to 240
- kv_down: bfloat16 [7168, 576], P('seq'), may hold values from -0.0625 to 0.0625
- kv_gain: float32 [512], replicated, may hold values from 0.25 to 1.75
- q_up: bfloat16 [1536, 24576], P(None, 'head'), may hold values from -0.15625 to 0.15625
- k_up: bfloat16 [512, 16384], P(None, 'head'), may hold values from -0.25 to 0.25
- v_up: bfloat16 [512, 16384], P(None, 'head'), may hold values from -0.25 to 0.25
- out_proj: bfloat16 [16384, 7168], P('head', 'seq'), may hold values from -0.125 to 0.125
- block_order: int32 [256], P('groups'), parts along dimension 0, may hold values from 0 to 63, each once
Outputs:
- attn_out: bfloat16 [6144, 7168], P(('groups', 'head', 'seq')), parts along dimension 0
The draws below stay inside these ranges and needn't reach their ends.
There are 4 independent parts, one for each index of `groups`. The reference program is written for one: setup_inputs(seed, part) draws one part's arguments, and reference() takes and returns one part's arrays. A program takes and returns all parts, laid end to end along the dimension named above; an argument that names none is the same for every part. Nothing has to cross between parts.
Inputs may be any that keep to these rules, and one draw needn't show every extreme that they name: Each of 0 to 63 once; stored rows j * 24 to (j + 1) * 24 - 1 hold the positions block_order[j] * 24 onwards, in order.
All inputs are finite; a program needn't handle non-finite values.
Results may differ from the reference program's by a relative error of at most 0.025.
Values may be sent and summed in bfloat16 or wider, within the bound.
No kernel may reach another device: no remote copies, remote signals or barrier semaphores. Data moves between devices by JAX's collectives and lax.ppermute only.
A program may use at most 128 MiB of HBM per device.

```python
import jax
import jax.numpy as jnp
from jax import lax

D = 7168
HEADS = 128
LATENT = 512
ROPE = 64
NOPE = 128
VDIM = 128
QLAT = 1536
TOK_DEV = 24
BLOCKS = 64
LENGTH = 1536
N_HEAD = 32


def draw_query_latent(key, part):
    key_base = jax.random.fold_in(key, 11)
    result = jnp.clip(2.0 * jax.random.normal(key_base, (LENGTH, QLAT), jnp.float32), -12.0, 12.0)
    return result.astype(jnp.bfloat16)


def block_scale(rng, shape, pieces, least, high):
    def one(axis_at, parts):
        steps = jax.random.uniform(jax.random.fold_in(jax.random.fold_in(rng, 6), axis_at), (parts,), jnp.float32, least / len(pieces), high / len(pieces))
        return jnp.repeat(jnp.exp(steps), shape[axis_at] // parts).reshape((-1,) + (1,) * (len(shape) - axis_at - 1))

    factor_of = one(*pieces[0])
    for cut in pieces[1:]:
        factor_of = factor_of * one(*cut)
    return factor_of


def bell_draw(key, dims, scale, reach, split=(), kind=jnp.bfloat16):
    values = jax.random.normal(key, dims, jnp.float32) * scale
    if len(split) > 0:
        values = block_scale(key, dims, split, -0.22, 0.18) * values
    return jnp.clip(values, min=-reach, max=reach).astype(kind)


def setup_inputs(seed: int = 0, part: int = 0) -> dict:
    keys = jax.random.split(jax.random.key(seed), 10)
    own_keys = jax.random.split(jax.random.fold_in(keys[9], part), 10)
    hidden = bell_draw(own_keys[0], (LENGTH, D), 1.0, 6.0, ((0, 64),))
    query_latent = draw_query_latent(jax.random.fold_in(jax.random.fold_in(keys[9], part), 71), part)
    kv_down = bell_draw(keys[2], (D, LATENT + ROPE), D ** -0.5, 0.0625, ((0, 2),))
    kv_gain = jnp.clip(1.0 + 0.15 * jax.random.normal(keys[3], (LATENT,), jnp.float32), 0.25, 1.75)
    q_up = bell_draw(keys[4], (QLAT, HEADS * (NOPE + ROPE)), QLAT ** -0.5, 0.15625, ((1, 32),))
    k_up = bell_draw(keys[5], (LATENT, HEADS * NOPE), LATENT ** -0.5, 0.25, ((1, 32),))
    v_up = bell_draw(keys[6], (LATENT, HEADS * VDIM), LATENT ** -0.5, 0.25, ((1, 32),))
    out_proj = bell_draw(keys[7], (HEADS * VDIM, D), (HEADS * VDIM // 8) ** -0.5, 0.125, ((0, 32), (1, 2)))
    block_order = jax.random.permutation(own_keys[8], BLOCKS).astype(jnp.int32)
    return {"hidden": hidden, "query_latent": query_latent, "kv_down": kv_down, "kv_gain": kv_gain, "q_up": q_up, "k_up": k_up, "v_up": v_up, "out_proj": out_proj, "block_order": block_order}


EPSILON = 1e-06
THETA = 10000.0
MASKED = -1e+30

def rotate(values, positions):
    half_width = values.shape[-1] // 2
    frequency = THETA ** (-jnp.arange(half_width, dtype=jnp.float32) / half_width)
    angles = positions.astype(jnp.float32)[:, None] * frequency[None, :]
    shaped = (values.shape[0],) + (1,) * (values.ndim - 2) + (half_width,)
    cosine = jnp.cos(angles).reshape(shaped)
    sine_table = jnp.sin(angles).reshape(shaped)
    front_part = values[..., :half_width]
    back_part = values[..., half_width:]
    return jnp.concatenate([front_part * cosine - back_part * sine_table, front_part * sine_table + back_part * cosine], axis=-1)

def reference(hidden, query_latent, kv_down, kv_gain, q_up, k_up, v_up, out_proj, block_order):
    row_index = jnp.arange(LENGTH, dtype=jnp.int32)
    positions = block_order[row_index // TOK_DEV] * TOK_DEV + row_index % TOK_DEV
    latent_raw = jnp.dot(hidden, kv_down, preferred_element_type=jnp.float32)
    compressed = latent_raw[:, :LATENT]
    mean_square = lax.optimization_barrier(jnp.mean(compressed * compressed, axis=-1, keepdims=True))
    kv_part = (compressed * lax.rsqrt(mean_square + EPSILON) * kv_gain).astype(jnp.bfloat16)
    rope_keys = rotate(latent_raw[:, LATENT:], positions).astype(jnp.bfloat16)
    scaling = (NOPE + ROPE) ** (-0.5)
    projected = jnp.dot(query_latent, q_up, preferred_element_type=jnp.float32).reshape(LENGTH, HEADS, NOPE + ROPE)
    queries = (jnp.concatenate([projected[..., :NOPE], rotate(projected[..., NOPE:], positions)], axis=-1) * scaling).astype(jnp.bfloat16)
    key_rows = jnp.dot(kv_part, k_up, preferred_element_type=jnp.float32).astype(jnp.bfloat16).reshape(LENGTH, HEADS, NOPE)
    value_rows = jnp.dot(kv_part, v_up, preferred_element_type=jnp.float32).astype(jnp.bfloat16).reshape(LENGTH, HEADS, VDIM)
    allowed = positions[None, :] <= positions[:, None]

    def one_head(operands):
        query_head, key_head, value_head = operands
        scores = jnp.dot(query_head[:, :NOPE], key_head.T, preferred_element_type=jnp.float32)
        scores = scores + jnp.dot(query_head[:, NOPE:], rope_keys.T, preferred_element_type=jnp.float32)
        scores = jnp.where(allowed, scores, MASKED)
        row_max = lax.optimization_barrier(jnp.max(scores, axis=-1, keepdims=True))
        weights = jnp.where(allowed, jnp.exp(scores - row_max), 0.0)
        totals = lax.optimization_barrier(jnp.sum(weights, axis=-1, keepdims=True))
        mixture = jnp.dot(weights.astype(jnp.bfloat16), value_head, preferred_element_type=jnp.float32) / totals
        return mixture.astype(jnp.bfloat16)
    heads_out = lax.map(one_head, (queries.transpose(1, 0, 2), key_rows.transpose(1, 0, 2), value_rows.transpose(1, 0, 2)))
    group_heads = HEADS // N_HEAD
    grouped_out = heads_out.reshape(N_HEAD, group_heads, LENGTH, VDIM)
    grouped_proj = out_proj.reshape(N_HEAD, group_heads * VDIM, D)

    def add_group(running, operands):
        head_block, proj_block = operands
        head_rows = head_block.transpose(1, 0, 2).reshape(LENGTH, group_heads * VDIM)
        partial_sum = jnp.dot(head_rows, proj_block, preferred_element_type=jnp.float32)
        rounded = lax.optimization_barrier(partial_sum.astype(jnp.bfloat16))
        return (running + rounded.astype(jnp.float32), None)
    summed, unused = lax.scan(add_group, jnp.zeros((LENGTH, D), jnp.float32), (grouped_out, grouped_proj))
    return summed.astype(jnp.bfloat16)
```

```python
import jax
import jax.numpy as jnp
from jax import lax
from jax.experimental import pallas as pl
from jax.experimental.pallas import tpu as pltpu
from jax.sharding import PartitionSpec as P


ROPE = 64
NOPE = 128
VDIM = 128

EPSILON = 1e-06
THETA = 10000.0
MASKED = -1e30
ROW_TILE = 192
CHUNK_PAIRS = 4
KEY_LANES = 256


def lookup(table, index):
    slots = jnp.arange(table.shape[0], dtype=jnp.int32)
    return jnp.sum(jnp.where(index[:, None] == slots[None, :], table[None, :], 0), axis=1)


def angles_of(positions, lanes, half_width):
    lane = jnp.arange(lanes, dtype=jnp.int32) % half_width
    frequency = THETA ** (-lane.astype(jnp.float32) / half_width)
    return positions.astype(jnp.float32)[:, None] * frequency[None, :]


def rotate(values, positions):
    half_width = values.shape[-1] // 2
    angles = angles_of(positions, half_width, half_width)
    cosine, sine = jnp.cos(angles), jnp.sin(angles)
    front, back = values[:, :half_width], values[:, half_width:]
    return jnp.concatenate([front * cosine - back * sine, front * sine + back * cosine], axis=-1)


def shift(x, axis, by):
    count = lax.axis_size(axis)
    return lax.ppermute(x, axis, [(i, (i + by) % count) for i in range(count)])


def attention_kernel(ql_ref, qup_ref, cos_ref, sin_ref, qpos_ref, kpos_ref, own_k, own_v, other_k, other_v, out_ref):
    projected = jnp.dot(ql_ref[...], qup_ref[...], preferred_element_type=jnp.float32)
    rows = projected.shape[0]
    count = own_k.shape[0]
    lane = lax.broadcasted_iota(jnp.int32, (rows, 128), 1)
    cosine, sine = cos_ref[...], sin_ref[...]
    front = (lane % ROPE) < ROPE // 2
    scaling = (NOPE + ROPE) ** (-0.5)
    tiles = []
    for t in range(3):
        x = projected[:, t * 128 : (t + 1) * 128]
        if t > 0:
            turned = jnp.where(front, -pltpu.roll(x, 128 - ROPE // 2, 1), pltpu.roll(x, ROPE // 2, 1))
            rotated = x * cosine + turned * sine
            x = jnp.where((lane < ROPE) if t == 1 else (lane >= ROPE), rotated, x)
        tiles.append((x * scaling).astype(jnp.bfloat16))
    for h in range(2):
        query = jnp.concatenate([tiles[h], tiles[h + 1]], axis=1)
        columns = slice(h * KEY_LANES, (h + 1) * KEY_LANES)
        scores = []
        for i, keys in enumerate((own_k, other_k)):
            part = lax.dot_general(
                query, keys[:, columns], (((1,), (1,)), ((), ())), preferred_element_type=jnp.float32
            )
            allowed = kpos_ref[:, i * count : (i + 1) * count] <= qpos_ref[...]
            scores.append(jnp.where(allowed, part, MASKED))
        largest = jnp.maximum(*(jnp.max(p, axis=-1, keepdims=True) for p in scores))
        total, mixed = 0.0, 0.0
        for part, values in zip(scores, (own_v, other_v)):
            weights = jnp.exp(part - largest)
            total = total + jnp.sum(weights, axis=-1, keepdims=True)
            mixed = mixed + jnp.dot(
                weights.astype(jnp.bfloat16),
                values[:, h * VDIM : (h + 1) * VDIM],
                preferred_element_type=jnp.float32,
            )
        out_ref[:, h * VDIM : (h + 1) * VDIM] = (mixed / total).astype(jnp.bfloat16)


def attend(gathered, q_up, cosine, sine, qpos, kpos, own, other, start, rows):
    depth = q_up.shape[0]
    pairs = own[1].shape[1] // (2 * VDIM)
    count = own[0].shape[0]
    pair_lanes = q_up.shape[1] // pairs
    tile = min(ROW_TILE, rows)
    by_row = lambda p, i: (start // tile + i, 0)
    by_pair = lambda p, i: (0, p)
    keys = pl.BlockSpec((count, 2 * KEY_LANES), by_pair)
    values = pl.BlockSpec((count, 2 * VDIM), by_pair)
    flops = 2 * rows * pairs * (depth * pair_lanes + 4 * count * (KEY_LANES + VDIM))
    return pl.pallas_call(
        attention_kernel,
        grid=(pairs, rows // tile),
        in_specs=[
            pl.BlockSpec((tile, depth), by_row),
            pl.BlockSpec((depth, pair_lanes), by_pair),
            pl.BlockSpec((tile, 128), by_row),
            pl.BlockSpec((tile, 128), by_row),
            pl.BlockSpec((tile, 1), by_row),
            pl.BlockSpec((1, 2 * count), lambda p, i: (0, 0)),
            keys,
            values,
            keys,
            values,
        ],
        out_specs=pl.BlockSpec((tile, 2 * VDIM), lambda p, i: (i, p)),
        out_shape=jax.ShapeDtypeStruct((rows, pairs * 2 * VDIM), jnp.bfloat16),
        cost_estimate=pl.CostEstimate(
            flops=flops,
            bytes_accessed=2 * (q_up.size + 2 * own[0].size + 2 * own[1].size + rows * depth),
            transcendentals=rows * pairs * 4 * count,
        ),
        compiler_params=pltpu.CompilerParams(vmem_limit_bytes=40 * 1024 * 1024),
        name="attention",
    )(gathered, q_up, cosine, sine, qpos, kpos, *own, *other)


def per_device(hidden, query_latent, kv_down, kv_gain, q_up, k_up, v_up, out_proj, block_order):
    tok_rows = hidden.shape[0]
    head_count = lax.axis_size("head")
    seq_count = lax.axis_size("seq")
    head_index = lax.axis_index("head")
    seq_index = lax.axis_index("seq")
    latent_width = kv_gain.shape[0]
    q_depth = query_latent.shape[1]
    heads_dev = v_up.shape[1] // VDIM
    half = head_count // 2

    other_proj = shift(out_proj, "seq", 1)

    own_block = head_index * seq_count + seq_index
    own_rows = jnp.arange(tok_rows, dtype=jnp.int32)
    own_pos = lookup(block_order, jnp.full((tok_rows,), own_block, jnp.int32)) * tok_rows + own_rows
    paired = lax.all_gather(hidden, "seq", axis=0, tiled=True)
    own_width = kv_down.shape[0]
    own_columns = lax.dynamic_slice_in_dim(paired, seq_index * own_width, own_width, 1)
    partial = jnp.dot(own_columns, kv_down, preferred_element_type=jnp.float32)
    blocks = partial.reshape(seq_count, tok_rows, partial.shape[1])
    latent_raw = lax.all_to_all(blocks, "seq", 0, 0, tiled=True).sum(axis=0)
    compressed = latent_raw[:, :latent_width]
    mean_square = jnp.mean(compressed * compressed, axis=-1, keepdims=True)
    kv_part = compressed * lax.rsqrt(mean_square + EPSILON) * kv_gain
    latent = jnp.concatenate(
        [kv_part, rotate(latent_raw[:, latent_width:], own_pos)], axis=1
    ).astype(jnp.bfloat16)

    held = {0: jnp.concatenate([query_latent, latent], axis=1)}
    up, down = held[0], held[0]
    for s in range(1, half + 1):
        up = shift(up, "head", 1)
        held[half if s == half else -s] = up
        if s < half:
            down = shift(down, "head", -1)
            held[s] = down
    order = []
    for s in range(half):
        order += [half - s, s - half + 1]
    gathered = jnp.concatenate([held[d] for d in order], axis=0)
    lat_own = gathered[:, q_depth:]
    lat_other = shift(lat_own, "seq", 1)

    query_count = gathered.shape[0]
    row = jnp.arange(query_count, dtype=jnp.int32)
    place = row // tok_rows
    relative = jnp.where(place % 2 == 0, half - place // 2, place // 2 - half + 1)
    owner = (head_index + relative + head_count) % head_count
    own_shard = lookup(block_order, owner * seq_count + seq_index) * tok_rows + row % tok_rows
    other_index = (seq_index + seq_count - 1) % seq_count
    other_shard = lookup(block_order, owner * seq_count + other_index) * tok_rows + row % tok_rows
    key_pos = jnp.concatenate([own_shard, other_shard])[None, :]
    query_pos = own_shard[:, None]
    angles = angles_of(own_shard, 128, ROPE // 2)
    cosine, sine = jnp.cos(angles), jnp.sin(angles)

    wide = []
    for h in range(heads_dev):
        part = jnp.pad(k_up[:, h * NOPE : (h + 1) * NOPE], ((0, ROPE), (0, 0)))
        zeros = jnp.zeros((part.shape[0], ROPE), part.dtype)
        unit = jnp.eye(part.shape[0], ROPE, k=-latent_width, dtype=part.dtype)
        wide += [part, unit, zeros] if h % 2 == 0 else [zeros, part, unit]
    k_wide = jnp.concatenate(wide, axis=1)

    def keys_values(lat):
        keys = jnp.dot(lat, k_wide, preferred_element_type=jnp.float32).astype(jnp.bfloat16)
        values = jnp.dot(lat[:, :latent_width], v_up, preferred_element_type=jnp.float32)
        return keys, values.astype(jnp.bfloat16)

    own, other = keys_values(lat_own), keys_values(lat_other)

    pieces = {}
    chunk = CHUNK_PAIRS * 2 * tok_rows
    for c in range(query_count // chunk):
        mixed = attend(
            gathered, q_up, cosine, sine, query_pos, key_pos, own, other, c * chunk, chunk
        )
        for g, weights in enumerate((out_proj, other_proj)):
            product = jnp.dot(mixed, weights, preferred_element_type=jnp.float32).astype(jnp.bfloat16)
            for i in range(2 * CHUNK_PAIRS):
                d = order[c * 2 * CHUNK_PAIRS + i]
                pieces[d, g] = product[i * tok_rows : (i + 1) * tok_rows]

    groups = range(2)
    right = [pieces[half, g] for g in groups]
    left = [pieces[1 - half, g] for g in groups]
    for s in range(1, half + 1):
        for g in groups:
            right[g] = shift(right[g], "head", 1)
            if s < half:
                left[g] = shift(left[g], "head", -1)
            if s < half:
                right[g] = (right[g].astype(jnp.float32) + pieces[half - s, g]).astype(jnp.bfloat16)
            if s < half - 1:
                left[g] = (left[g].astype(jnp.float32) + pieces[s + 1 - half, g]).astype(jnp.bfloat16)
    sums = [
        (right[g].astype(jnp.float32) + left[g] + pieces[0, g]).astype(jnp.bfloat16) for g in groups
    ]
    first = seq_index == 0
    return jnp.concatenate(
        [jnp.where(first, sums[0], sums[1]), jnp.where(first, sums[1], sums[0])], axis=1
    )


def solution(mesh):
    placed = (
        P(("groups", "head", "seq"), None),
        P(("groups", "head", "seq"), None),
        P("seq", None),
        P(),
        P(None, "head"),
        P(None, "head"),
        P(None, "head"),
        P("head", "seq"),
        P("groups"),
    )
    return jax.shard_map(
        per_device,
        mesh=mesh,
        in_specs=placed,
        out_specs=P(("groups", "head", "seq"), None),
        check_vma=False,
    )
```
